32 devices in a mesh: gy: 8 (over z, x), gx: 4 (over y, core).
Axes of the slice: x: 2, y: 2, z: 4, core: 2. Of those that a mesh axis runs over, the one named last changes fastest.
Arguments:
- fields: float32 [8, 64, 256, 128], P(None, 'gx', 'gy'), may hold values from -6 to 6
- shifts: int32 [64], P('gx'), may hold values from 0 to 255
- fraction: float32 [64], P('gx'), may hold values from 0.4 to 0.6
Outputs:
- remapped: float32 [8, 64, 256, 128], P(None, 'gx', 'gy')
- stress: float32 [2, 128], replicated
The draws below stay inside these ranges and needn't reach their ends.
All inputs are finite; a program needn't handle non-finite values.
Results may differ from the reference program's by a relative error of at most 0.0003.
Values sent between devices are 32-bit elements; how exact they have to be, the bound alone decides.
A program may use at most 64 MiB of HBM per device.

```python
import math
import jax
import jax.numpy as jnp
from jax import lax

FIELDS = 8
CZ = 128
NX = 64
NY = 256


def draw_fields(key, part):
    key_rough = jax.random.fold_in(key, 11)
    key_level = jax.random.fold_in(key, 12)
    rough_part = jnp.clip(jax.random.normal(key_rough, (FIELDS, NX, NY, CZ), jnp.float32), -5.0, 5.0)
    amplitude = jax.random.uniform(key_level, (2, NX, 1, CZ), jnp.float32, 0.3, 0.6)
    parity = 1.0 - 2.0 * (jnp.arange(NY) % 2).astype(jnp.float32)
    alternating = amplitude * parity[None, None, :, None]
    component = jnp.arange(FIELDS)
    first_pair = ((component == 1) | (component == 2)).astype(jnp.float32)
    second_pair = ((component == 5) | (component == 6)).astype(jnp.float32)
    pattern = first_pair[:, None, None, None] * alternating[0][None] + second_pair[:, None, None, None] * alternating[1][None]
    return rough_part + pattern


def place_ends(array, key, smallest, high):
    longest = array.shape.index(max(array.shape))
    spots = []
    for shift in (0, 1):
        where = [jax.random.randint(jax.random.fold_in(key, axis), (), 0, length) for axis, length in enumerate(array.shape)]
        where[longest] = (where[longest] + shift) % array.shape[longest]
        spots.append(tuple(where))
    return array.at[spots[0]].set(smallest).at[spots[1]].set(high)


def steps_of(key, dims, shards, least, high):
    gain, own = 1.0, jax.random.fold_in(key, 6)
    for axis_at, blocks in shards:
        steps = jnp.exp(jax.random.uniform(jax.random.fold_in(own, axis_at), (blocks,), jnp.float32, least / len(shards), high / len(shards)))
        gain = gain * jnp.repeat(steps, dims[axis_at] // blocks).reshape([-1 if axis == axis_at else 1 for axis in range(len(dims))])
    return gain


def setup_inputs(seed: int = 0) -> dict:
    key_of = jax.random.split(jax.random.key(seed), 4)
    return {
        "fields": draw_fields(jax.random.fold_in(key_of[3], 71), 0),
        "shifts": place_ends(jax.random.randint(key_of[1], (NX,), 0, NY), jax.random.fold_in(key_of[1], 1), 0, NY - 1).astype(jnp.int32),
        "fraction": jnp.clip(0.4 + 0.20000002 * jax.random.uniform(key_of[2], (NX,), jnp.float32) ** steps_of(key_of[2], (NX,), ((0, 4),), -0.2, 0.2), 0.4, 0.6),
    }


def remap_cells(extended, fraction, length, stride):

    def cells(first, number):
        return extended[..., first * stride:(first + number) * stride]
    interface = (7.0 * (cells(1, length + 2) + cells(2, length + 2)) - (cells(0, length + 2) + cells(3, length + 2))) / 12.0
    left_edge = interface[..., :(length + 1) * stride]
    right_edge = interface[..., stride:]
    centre = cells(2, length + 1)
    slope = right_edge - left_edge
    curve = 6.0 * centre - 3.0 * (left_edge + right_edge)
    outflow = fraction * (right_edge - 0.5 * fraction * (slope - (1.0 - 2.0 * fraction / 3.0) * curve))
    return cells(3, length) - outflow[..., stride:] + outflow[..., :length * stride]

def reference(fields, shifts, fraction):

    def one_column(items):
        column, shift, share = items
        start = jnp.mod(-3 - shift, NY).astype(jnp.int32)
        doubled = jnp.concatenate([column, column, column[:, :4, :]], axis=1)
        extended = lax.dynamic_slice_in_dim(doubled, start, NY + 5, 1)
        flat = extended.reshape(FIELDS, (NY + 5) * CZ)
        return remap_cells(flat, share, NY, CZ).reshape(FIELDS, NY, CZ)
    moved = lax.map(one_column, (jnp.moveaxis(fields, 1, 0), shifts, fraction))
    remapped = jnp.moveaxis(moved, 0, 1)
    reynolds = lax.optimization_barrier(jnp.sum(remapped[1] * remapped[2], axis=(0, 1)))
    maxwell = -lax.optimization_barrier(jnp.sum(remapped[5] * remapped[6], axis=(0, 1)))
    stress = jnp.stack([reynolds, maxwell]) / math.sqrt(NX * NY)
    return (remapped, stress)
```

```python
from functools import partial
import math

import jax
import jax.numpy as jnp
from jax import lax
from jax.experimental import pallas as pl
from jax.experimental.pallas import tpu as pltpu
from jax.sharding import PartitionSpec as P

MESH = pl.DeviceIdType.MESH
FIRST_FIELDS = (1, 2, 5, 6)
TILE = 32
PAD = TILE + 8


def taps_of(share):
    half = 0.5 * share * share
    bend = half * (1.0 - 2.0 * share / 3.0)
    right = (share - half - 3.0 * bend) * (1.0 / 12.0)
    left = (half - 3.0 * bend) * (1.0 / 12.0)
    return (
        -left,
        8.0 * left - right,
        8.0 * right + 6.0 * bend,
        1.0 - 8.0 * left - 6.0 * bend,
        left - 8.0 * right,
        right,
    )


def kernel(
    plan, shifts, fraction, fields, remapped, stress, held, moved, part, part_y,
    sums, part_x, send1, recv1, send2, recv2, ysend, yrecv, xsend, xrecv,
):
    n, m, components, chunks, depth, per_device, slab, azimuth, scale = plan
    me = lax.axis_index("gy")
    my_x = lax.axis_index("gx")
    order = FIRST_FIELDS + tuple(
        f for f in range(components) if f not in FIRST_FIELDS
    )

    def column_of(device):
        return device * per_device // components

    def field_of(device, chunk):
        if per_device >= components:
            return order[chunk]
        return lax.rem(lax.rem(device * per_device, components) + chunk + 1, components)

    def peer(step):
        return lax.rem(me + step, n)

    barrier = pltpu.get_barrier_semaphore()

    def greet_y(step, carry):
        pl.semaphore_signal(
            barrier, inc=1, device_id={"gy": peer(step)}, device_id_type=MESH
        )
        return carry

    lax.fori_loop(1, n, greet_y, 0)
    for step in range(1, m):
        pl.semaphore_signal(
            barrier,
            inc=1,
            device_id={"gx": lax.rem(my_x + step, m)},
            device_id_type=MESH,
        )

    def own_in(chunk):
        return pltpu.make_async_copy(
            fields.at[field_of(me, chunk), pl.ds(column_of(me), depth)],
            held[chunk].at[:, pl.ds(me * slab, slab)],
            recv1.at[chunk],
        )

    for chunk in range(chunks):
        own_in(chunk).start()
    pl.semaphore_wait(barrier, n - 1 + m - 1)

    for chunk in range(chunks):

        def send_in(step, carry):
            to = peer(step)
            pltpu.make_async_remote_copy(
                src_ref=fields.at[field_of(to, chunk), pl.ds(column_of(to), depth)],
                dst_ref=held[chunk].at[:, pl.ds(me * slab, slab)],
                send_sem=send1.at[chunk],
                recv_sem=recv1.at[chunk],
                device_id={"gy": to},
                device_id_type=MESH,
            ).start()
            return carry

        lax.fori_loop(1, n, send_in, 0)

    def whole(chunk):
        return held[chunk].at[:, pl.ds(0, azimuth)]

    def others(chunk):
        return held[chunk].at[:, pl.ds(0, azimuth - slab)]

    def remap(chunk):
        for c in range(depth):
            column = column_of(me) + c
            shift = shifts[column]
            taps = taps_of(fraction[column])
            held[chunk][c, pl.ds(azimuth, PAD)] = held[chunk][c, pl.ds(0, PAD)]

            def tile(t, carry):
                start = lax.rem(t * TILE - 3 - shift + 2 * azimuth, azimuth)
                total = None
                for k in range(6):
                    term = taps[k] * held[chunk][c, pl.ds(start + k, TILE)]
                    total = term if total is None else total + term
                moved[chunk, c, pl.ds(pl.multiple_of(t * TILE, TILE), TILE)] = total
                return carry

            lax.fori_loop(0, azimuth // TILE, tile, 0)

    def own_out(chunk):
        return pltpu.make_async_copy(
            moved.at[chunk, :, pl.ds(me * slab, slab)],
            remapped.at[field_of(me, chunk), pl.ds(column_of(me), depth)],
            recv2.at[chunk],
        )

    def pair_sum(chunk):
        def add(t, total):
            rows = pl.ds(pl.multiple_of(t * 8, 8), 8)
            for c in range(depth):
                total = total + moved[chunk, c, rows] * moved[chunk + 1, c, rows]
            return total

        total = lax.fori_loop(
            0, azimuth // 8, add, jnp.zeros((8, moved.shape[-1]), jnp.float32)
        )
        return jnp.sum(total, axis=0, keepdims=True)

    def start_sums():
        part[...] = jnp.zeros(part.shape, jnp.float32)
        if per_device >= components:
            part[0:1] = pair_sum(0)
            part[1:2] = -pair_sum(2)
        else:
            first = jnp.zeros((1, moved.shape[-1]), jnp.float32)
            second = first
            for chunk in range(0, chunks, 2):
                total = pair_sum(chunk)
                field = field_of(me, chunk)
                first = first + jnp.where(field == 1, total, 0.0)
                second = second - jnp.where(field == 5, total, 0.0)
            part[0:1] = first
            part[1:2] = second
        part_y[pl.ds(me, 1)] = part[...][None]

        def send_sum(step, carry):
            pltpu.make_async_remote_copy(
                src_ref=part,
                dst_ref=part_y.at[me],
                send_sem=ysend,
                recv_sem=yrecv,
                device_id={"gy": peer(step)},
                device_id_type=MESH,
            ).start()
            return carry

        lax.fori_loop(1, n, send_sum, 0)

    sums_at = min(3, chunks - 1) if per_device >= components else chunks - 1
    for chunk in range(chunks):
        pltpu.make_async_copy(whole(chunk), whole(chunk), recv1.at[chunk]).wait()
        remap(chunk)

        def send_out(step, carry):
            to = peer(step)
            pltpu.make_async_remote_copy(
                src_ref=moved.at[chunk, :, pl.ds(to * slab, slab)],
                dst_ref=remapped.at[field_of(me, chunk), pl.ds(column_of(me), depth)],
                send_sem=send2.at[chunk],
                recv_sem=recv2.at[chunk],
                device_id={"gy": to},
                device_id_type=MESH,
            ).start()
            return carry

        lax.fori_loop(1, n, send_out, 0)
        own_out(chunk).start()
        if chunk == sums_at:
            start_sums()

    few = part_y.at[pl.ds(0, n - 1)]
    pltpu.make_async_copy(few, few, yrecv).wait()
    pltpu.make_async_copy(few, few, ysend).wait()
    sums[...] = jnp.sum(part_y[...], axis=0)
    part_x[pl.ds(my_x, 1)] = sums[...][None]
    for step in range(1, m):
        pltpu.make_async_remote_copy(
            src_ref=sums,
            dst_ref=part_x.at[my_x],
            send_sem=xsend,
            recv_sem=xrecv,
            device_id={"gx": lax.rem(my_x + step, m)},
            device_id_type=MESH,
        ).start()
    rest = part_x.at[pl.ds(0, m - 1)]
    pltpu.make_async_copy(rest, rest, xrecv).wait()
    pltpu.make_async_copy(rest, rest, xsend).wait()
    stress[...] = jnp.sum(part_x[...], axis=0)[0:2] * scale

    for chunk in range(chunks):
        pltpu.make_async_copy(others(chunk), others(chunk), send1.at[chunk]).wait()
        pltpu.make_async_copy(others(chunk), others(chunk), send2.at[chunk]).wait()
        pltpu.make_async_copy(whole(chunk), whole(chunk), recv2.at[chunk]).wait()


def on_device(fields, shifts, fraction):
    components, columns, slab, vertical = fields.shape
    n = lax.axis_size("gy")
    m = lax.axis_size("gx")
    azimuth = slab * n
    per_device = components * columns // n
    chunks = min(per_device, components)
    depth = max(1, per_device // components)
    scale = 1.0 / math.sqrt(columns * m * azimuth)
    plan = (n, m, components, chunks, depth, per_device, slab, azimuth, scale)
    DMA = pltpu.SemaphoreType.DMA
    return pl.pallas_call(
        partial(kernel, plan),
        out_shape=(
            jax.ShapeDtypeStruct(fields.shape, jnp.float32),
            jax.ShapeDtypeStruct((2, vertical), jnp.float32),
        ),
        in_specs=[
            pl.BlockSpec(memory_space=pltpu.SMEM),
            pl.BlockSpec(memory_space=pltpu.SMEM),
            pl.BlockSpec(memory_space=pl.ANY),
        ],
        out_specs=(
            pl.BlockSpec(memory_space=pl.ANY),
            pl.BlockSpec(memory_space=pltpu.VMEM),
        ),
        scratch_shapes=[
            [pltpu.VMEM((depth, azimuth + PAD, vertical), jnp.float32)] * chunks,
            pltpu.VMEM((chunks, depth, azimuth, vertical), jnp.float32),
            pltpu.VMEM((8, vertical), jnp.float32),
            pltpu.VMEM((n, 8, vertical), jnp.float32),
            pltpu.VMEM((8, vertical), jnp.float32),
            pltpu.VMEM((m, 8, vertical), jnp.float32),
            DMA((chunks,)),
            DMA((chunks,)),
            DMA((chunks,)),
            DMA((chunks,)),
            DMA,
            DMA,
            DMA,
            DMA,
        ],
        compiler_params=pltpu.CompilerParams(collective_id=0, has_side_effects=True),
        cost_estimate=pl.CostEstimate(
            flops=12 * fields.size, bytes_accessed=8 * fields.size, transcendentals=0
        ),
    )(shifts, fraction, fields)


def solution(mesh):
    in_specs = (P(None, "gx", "gy", None), P("gx"), P("gx"))
    out_specs = (P(None, "gx", "gy", None), P())
    return jax.shard_map(
        on_device, mesh=mesh, in_specs=in_specs, out_specs=out_specs, check_vma=False
    )
```

```python
from functools import partial
import math

import jax
import jax.numpy as jnp
from jax import lax
from jax.experimental import pallas as pl
from jax.experimental.pallas import tpu as pltpu
from jax.sharding import PartitionSpec as P

MESH = pl.DeviceIdType.MESH
FIRST_FIELDS = (1, 2, 5, 6)
TILE = 32
PAD = TILE + 8


def taps_of(share):
    half = 0.5 * share * share
    bend = half * (1.0 - 2.0 * share / 3.0)
    right = (share - half - 3.0 * bend) * (1.0 / 12.0)
    left = (half - 3.0 * bend) * (1.0 / 12.0)
    return (
        -left,
        8.0 * left - right,
        8.0 * right + 6.0 * bend,
        1.0 - 8.0 * left - 6.0 * bend,
        left - 8.0 * right,
        right,
    )


def kernel(
    plan, shifts_in, fraction_in, fields, remapped, stress, held, moved, part, part_y,
    sums, part_x, send1, recv1, send2, recv2, ysend, yrecv, xsend, xrecv, shifts,
    fraction, small_sem,
):
    n, m, components, chunks, depth, per_device, slab, azimuth, scale = plan
    me = lax.axis_index("gy")
    my_x = lax.axis_index("gx")
    order = FIRST_FIELDS + tuple(
        f for f in range(components) if f not in FIRST_FIELDS
    )

    def column_of(device):
        return device * per_device // components

    def field_of(device, chunk):
        if per_device >= components:
            return order[chunk]
        return lax.rem(lax.rem(device * per_device, components) + chunk + 1, components)

    def peer(step):
        return lax.rem(me + step, n)

    small = (
        pltpu.make_async_copy(shifts_in, shifts, small_sem.at[0]),
        pltpu.make_async_copy(fraction_in, fraction, small_sem.at[1]),
    )
    barrier = pltpu.get_barrier_semaphore()

    def greet_y(step, carry):
        pl.semaphore_signal(
            barrier, inc=1, device_id={"gy": peer(step)}, device_id_type=MESH
        )
        return carry

    lax.fori_loop(1, n, greet_y, 0)
    for step in range(1, m):
        pl.semaphore_signal(
            barrier,
            inc=1,
            device_id={"gx": lax.rem(my_x + step, m)},
            device_id_type=MESH,
        )

    def own_in(chunk):
        return pltpu.make_async_copy(
            fields.at[field_of(me, chunk), pl.ds(column_of(me), depth)],
            held[chunk].at[:, pl.ds(me * slab, slab)],
            recv1.at[chunk],
        )

    for copy in small:
        copy.start()
    for chunk in range(chunks):
        own_in(chunk).start()
    pl.semaphore_wait(barrier, n - 1 + m - 1)

    for chunk in range(chunks):

        def send_in(step, carry):
            to = peer(step)
            pltpu.make_async_remote_copy(
                src_ref=fields.at[field_of(to, chunk), pl.ds(column_of(to), depth)],
                dst_ref=held[chunk].at[:, pl.ds(me * slab, slab)],
                send_sem=send1.at[chunk],
                recv_sem=recv1.at[chunk],
                device_id={"gy": to},
                device_id_type=MESH,
            ).start()
            return carry

        lax.fori_loop(1, n, send_in, 0)

    def whole(chunk):
        return held[chunk].at[:, pl.ds(0, azimuth)]

    def others(chunk):
        return held[chunk].at[:, pl.ds(0, azimuth - slab)]

    def remap(chunk):
        for c in range(depth):
            column = column_of(me) + c
            shift = shifts[column]
            taps = taps_of(fraction[column])
            held[chunk][c, pl.ds(azimuth, PAD)] = held[chunk][c, pl.ds(0, PAD)]

            def tile(t, carry):
                start = lax.rem(t * TILE - 3 - shift + 2 * azimuth, azimuth)
                total = None
                for k in range(6):
                    term = taps[k] * held[chunk][c, pl.ds(start + k, TILE)]
                    total = term if total is None else total + term
                moved[chunk, c, pl.ds(pl.multiple_of(t * TILE, TILE), TILE)] = total
                return carry

            lax.fori_loop(0, azimuth // TILE, tile, 0)

    def own_out(chunk):
        return pltpu.make_async_copy(
            moved.at[chunk, :, pl.ds(me * slab, slab)],
            remapped.at[field_of(me, chunk), pl.ds(column_of(me), depth)],
            recv2.at[chunk],
        )

    def pair_sum(chunk):
        def add(t, total):
            rows = pl.ds(pl.multiple_of(t * 8, 8), 8)
            for c in range(depth):
                total = total + moved[chunk, c, rows] * moved[chunk + 1, c, rows]
            return total

        total = lax.fori_loop(
            0, azimuth // 8, add, jnp.zeros((8, moved.shape[-1]), jnp.float32)
        )
        return jnp.sum(total, axis=0, keepdims=True)

    def start_sums():
        part[...] = jnp.zeros(part.shape, jnp.float32)
        if per_device >= components:
            part[0:1] = pair_sum(0)
            part[1:2] = -pair_sum(2)
        else:
            first = jnp.zeros((1, moved.shape[-1]), jnp.float32)
            second = first
            for chunk in range(0, chunks, 2):
                total = pair_sum(chunk)
                field = field_of(me, chunk)
                first = first + jnp.where(field == 1, total, 0.0)
                second = second - jnp.where(field == 5, total, 0.0)
            part[0:1] = first
            part[1:2] = second
        part_y[pl.ds(me, 1)] = part[...][None]

        def send_sum(step, carry):
            pltpu.make_async_remote_copy(
                src_ref=part,
                dst_ref=part_y.at[me],
                send_sem=ysend,
                recv_sem=yrecv,
                device_id={"gy": peer(step)},
                device_id_type=MESH,
            ).start()
            return carry

        lax.fori_loop(1, n, send_sum, 0)

    for copy in small:
        copy.wait()
    sums_at = min(3, chunks - 1) if per_device >= components else chunks - 1
    for chunk in range(chunks):
        pltpu.make_async_copy(whole(chunk), whole(chunk), recv1.at[chunk]).wait()
        remap(chunk)

        def send_out(step, carry):
            to = peer(step)
            pltpu.make_async_remote_copy(
                src_ref=moved.at[chunk, :, pl.ds(to * slab, slab)],
                dst_ref=remapped.at[field_of(me, chunk), pl.ds(column_of(me), depth)],
                send_sem=send2.at[chunk],
                recv_sem=recv2.at[chunk],
                device_id={"gy": to},
                device_id_type=MESH,
            ).start()
            return carry

        lax.fori_loop(1, n, send_out, 0)
        own_out(chunk).start()
        if chunk == sums_at:
            start_sums()

    few = part_y.at[pl.ds(0, n - 1)]
    pltpu.make_async_copy(few, few, yrecv).wait()
    pltpu.make_async_copy(few, few, ysend).wait()
    sums[...] = jnp.sum(part_y[...], axis=0)
    part_x[pl.ds(my_x, 1)] = sums[...][None]
    for step in range(1, m):
        pltpu.make_async_remote_copy(
            src_ref=sums,
            dst_ref=part_x.at[my_x],
            send_sem=xsend,
            recv_sem=xrecv,
            device_id={"gx": lax.rem(my_x + step, m)},
            device_id_type=MESH,
        ).start()
    rest = part_x.at[pl.ds(0, m - 1)]
    pltpu.make_async_copy(rest, rest, xrecv).wait()
    pltpu.make_async_copy(rest, rest, xsend).wait()
    stress[...] = jnp.sum(part_x[...], axis=0)[0:2] * scale

    for chunk in range(chunks):
        pltpu.make_async_copy(others(chunk), others(chunk), send1.at[chunk]).wait()
        pltpu.make_async_copy(others(chunk), others(chunk), send2.at[chunk]).wait()
        pltpu.make_async_copy(whole(chunk), whole(chunk), recv2.at[chunk]).wait()


def on_device(fields, shifts, fraction):
    components, columns, slab, vertical = fields.shape
    n = lax.axis_size("gy")
    m = lax.axis_size("gx")
    azimuth = slab * n
    per_device = components * columns // n
    chunks = min(per_device, components)
    depth = max(1, per_device // components)
    scale = 1.0 / math.sqrt(columns * m * azimuth)
    plan = (n, m, components, chunks, depth, per_device, slab, azimuth, scale)
    DMA = pltpu.SemaphoreType.DMA
    return pl.pallas_call(
        partial(kernel, plan),
        out_shape=(
            jax.ShapeDtypeStruct(fields.shape, jnp.float32),
            jax.ShapeDtypeStruct((2, vertical), jnp.float32),
        ),
        in_specs=[
            pl.BlockSpec(memory_space=pltpu.HBM),
            pl.BlockSpec(memory_space=pltpu.HBM),
            pl.BlockSpec(memory_space=pltpu.HBM),
        ],
        out_specs=(
            pl.BlockSpec(memory_space=pl.ANY),
            pl.BlockSpec(memory_space=pltpu.VMEM),
        ),
        scratch_shapes=[
            [pltpu.VMEM((depth, azimuth + PAD, vertical), jnp.float32)] * chunks,
            pltpu.VMEM((chunks, depth, azimuth, vertical), jnp.float32),
            pltpu.VMEM((8, vertical), jnp.float32),
            pltpu.VMEM((n, 8, vertical), jnp.float32),
            pltpu.VMEM((8, vertical), jnp.float32),
            pltpu.VMEM((m, 8, vertical), jnp.float32),
            DMA((chunks,)),
            DMA((chunks,)),
            DMA((chunks,)),
            DMA((chunks,)),
            DMA,
            DMA,
            DMA,
            DMA,
            pltpu.SMEM((columns,), jnp.int32),
            pltpu.SMEM((columns,), jnp.float32),
            DMA((2,)),
        ],
        compiler_params=pltpu.CompilerParams(
            collective_id=0, has_side_effects=True, vmem_limit_bytes=16 * 2**20
        ),
        cost_estimate=pl.CostEstimate(
            flops=12 * fields.size, bytes_accessed=8 * fields.size, transcendentals=0
        ),
    )(*(pltpu.with_memory_space_constraint(a, pltpu.HBM) for a in (shifts, fraction, fields)))


def solution(mesh):
    in_specs = (P(None, "gx", "gy", None), P("gx"), P("gx"))
    out_specs = (P(None, "gx", "gy", None), P())
    return jax.shard_map(
        on_device, mesh=mesh, in_specs=in_specs, out_specs=out_specs, check_vma=False
    )
```

```python
from functools import partial
import math

import jax
import jax.numpy as jnp
from jax import lax
from jax.experimental import pallas as pl
from jax.experimental.pallas import tpu as pltpu
from jax.sharding import PartitionSpec as P

MESH = pl.DeviceIdType.MESH
FIRST_FIELDS = (1, 2, 5, 6)
TILE = 32
PAD = TILE + 8


def taps_of(share):
    half = 0.5 * share * share
    bend = half * (1.0 - 2.0 * share / 3.0)
    right = (share - half - 3.0 * bend) * (1.0 / 12.0)
    left = (half - 3.0 * bend) * (1.0 / 12.0)
    return (
        -left,
        8.0 * left - right,
        8.0 * right + 6.0 * bend,
        1.0 - 8.0 * left - 6.0 * bend,
        left - 8.0 * right,
        right,
    )


def kernel(
    plan, shifts_in, fraction_in, fields, remapped, stress, held, moved, part, part_y,
    sums, part_x, send1, recv1, send2, recv2, ysend, yrecv, xsend, xrecv, shifts,
    fraction, small_sem,
):
    n, m, components, chunks, depth, per_device, slab, azimuth, scale = plan
    me = lax.axis_index("gy")
    my_x = lax.axis_index("gx")
    order = FIRST_FIELDS + tuple(
        f for f in range(components) if f not in FIRST_FIELDS
    )

    def column_of(device):
        return device * per_device // components

    def field_of(device, chunk):
        if per_device >= components:
            return order[chunk]
        return lax.rem(lax.rem(device * per_device, components) + chunk + 1, components)

    def peer(step):
        away = lax.div(step, 2) * (1 - 2 * lax.rem(step, 2))
        return lax.rem(me + n // 2 + away, n)

    small = (
        pltpu.make_async_copy(shifts_in, shifts, small_sem.at[0]),
        pltpu.make_async_copy(fraction_in, fraction, small_sem.at[1]),
    )
    barrier = pltpu.get_barrier_semaphore()

    def greet_y(step, carry):
        pl.semaphore_signal(
            barrier, inc=1, device_id={"gy": peer(step)}, device_id_type=MESH
        )
        return carry

    lax.fori_loop(1, n, greet_y, 0)
    for step in range(1, m):
        pl.semaphore_signal(
            barrier,
            inc=1,
            device_id={"gx": lax.rem(my_x + step, m)},
            device_id_type=MESH,
        )

    def own_in(chunk):
        return pltpu.make_async_copy(
            fields.at[field_of(me, chunk), pl.ds(column_of(me), depth)],
            held[chunk].at[:, pl.ds(me * slab, slab)],
            recv1.at[chunk],
        )

    for copy in small:
        copy.start()
    for chunk in range(chunks):
        own_in(chunk).start()
    pl.semaphore_wait(barrier, n - 1 + m - 1)

    for chunk in range(chunks):

        def send_in(step, carry):
            to = peer(step)
            pltpu.make_async_remote_copy(
                src_ref=fields.at[field_of(to, chunk), pl.ds(column_of(to), depth)],
                dst_ref=held[chunk].at[:, pl.ds(me * slab, slab)],
                send_sem=send1.at[chunk],
                recv_sem=recv1.at[chunk],
                device_id={"gy": to},
                device_id_type=MESH,
            ).start()
            return carry

        lax.fori_loop(1, n, send_in, 0)

    def whole(chunk):
        return held[chunk].at[:, pl.ds(0, azimuth)]

    def others(chunk):
        return held[chunk].at[:, pl.ds(0, azimuth - slab)]

    def remap(chunk):
        for c in range(depth):
            column = column_of(me) + c
            shift = shifts[column]
            taps = taps_of(fraction[column])
            held[chunk][c, pl.ds(azimuth, PAD)] = held[chunk][c, pl.ds(0, PAD)]

            def tile(t, carry):
                start = lax.rem(t * TILE - 3 - shift + 2 * azimuth, azimuth)
                total = None
                for k in range(6):
                    term = taps[k] * held[chunk][c, pl.ds(start + k, TILE)]
                    total = term if total is None else total + term
                moved[chunk, c, pl.ds(pl.multiple_of(t * TILE, TILE), TILE)] = total
                return carry

            lax.fori_loop(0, azimuth // TILE, tile, 0)

    def own_out(chunk):
        return pltpu.make_async_copy(
            moved.at[chunk, :, pl.ds(me * slab, slab)],
            remapped.at[field_of(me, chunk), pl.ds(column_of(me), depth)],
            recv2.at[chunk],
        )

    def pair_sum(chunk):
        def add(t, total):
            rows = pl.ds(pl.multiple_of(t * 8, 8), 8)
            for c in range(depth):
                total = total + moved[chunk, c, rows] * moved[chunk + 1, c, rows]
            return total

        total = lax.fori_loop(
            0, azimuth // 8, add, jnp.zeros((8, moved.shape[-1]), jnp.float32)
        )
        return jnp.sum(total, axis=0, keepdims=True)

    def start_sums():
        if per_device >= components:
            part[0:1] = pair_sum(0)
            part[1:2] = -pair_sum(2)
        else:
            first = jnp.zeros((1, moved.shape[-1]), jnp.float32)
            second = first
            for chunk in range(0, chunks, 2):
                total = pair_sum(chunk)
                field = field_of(me, chunk)
                first = first + jnp.where(field == 1, total, 0.0)
                second = second - jnp.where(field == 5, total, 0.0)
            part[0:1] = first
            part[1:2] = second
        part_y[pl.ds(me, 1)] = part[...][None]

        def send_sum(step, carry):
            pltpu.make_async_remote_copy(
                src_ref=part,
                dst_ref=part_y.at[me],
                send_sem=ysend,
                recv_sem=yrecv,
                device_id={"gy": peer(step)},
                device_id_type=MESH,
            ).start()
            return carry

        lax.fori_loop(1, n, send_sum, 0)

    for copy in small:
        copy.wait()
    sums_at = min(3, chunks - 1) if per_device >= components else chunks - 1
    for chunk in range(chunks):
        pltpu.make_async_copy(whole(chunk), whole(chunk), recv1.at[chunk]).wait()
        remap(chunk)

        def send_out(step, carry):
            to = peer(step)
            pltpu.make_async_remote_copy(
                src_ref=moved.at[chunk, :, pl.ds(to * slab, slab)],
                dst_ref=remapped.at[field_of(me, chunk), pl.ds(column_of(me), depth)],
                send_sem=send2.at[chunk],
                recv_sem=recv2.at[chunk],
                device_id={"gy": to},
                device_id_type=MESH,
            ).start()
            return carry

        lax.fori_loop(1, n, send_out, 0)
        own_out(chunk).start()
        if chunk == sums_at:
            start_sums()

    few = part_y.at[pl.ds(0, n - 1)]
    pltpu.make_async_copy(few, few, yrecv).wait()
    pltpu.make_async_copy(few, few, ysend).wait()
    sums[...] = jnp.sum(part_y[...], axis=0)
    part_x[pl.ds(my_x, 1)] = sums[...][None]
    for step in range(1, m):
        pltpu.make_async_remote_copy(
            src_ref=sums,
            dst_ref=part_x.at[my_x],
            send_sem=xsend,
            recv_sem=xrecv,
            device_id={"gx": lax.rem(my_x + step, m)},
            device_id_type=MESH,
        ).start()
    rest = part_x.at[pl.ds(0, m - 1)]
    pltpu.make_async_copy(rest, rest, xrecv).wait()
    pltpu.make_async_copy(rest, rest, xsend).wait()
    stress[...] = jnp.sum(part_x[...], axis=0) * scale

    for chunk in range(chunks):
        pltpu.make_async_copy(others(chunk), others(chunk), send1.at[chunk]).wait()
        pltpu.make_async_copy(others(chunk), others(chunk), send2.at[chunk]).wait()
        pltpu.make_async_copy(whole(chunk), whole(chunk), recv2.at[chunk]).wait()


def on_device(fields, shifts, fraction):
    components, columns, slab, vertical = fields.shape
    n = lax.axis_size("gy")
    m = lax.axis_size("gx")
    azimuth = slab * n
    per_device = components * columns // n
    chunks = min(per_device, components)
    depth = max(1, per_device // components)
    scale = 1.0 / math.sqrt(columns * m * azimuth)
    plan = (n, m, components, chunks, depth, per_device, slab, azimuth, scale)
    DMA = pltpu.SemaphoreType.DMA
    return pl.pallas_call(
        partial(kernel, plan),
        out_shape=(
            jax.ShapeDtypeStruct(fields.shape, jnp.float32),
            jax.ShapeDtypeStruct((2, vertical), jnp.float32),
        ),
        in_specs=[
            pl.BlockSpec(memory_space=pltpu.HBM),
            pl.BlockSpec(memory_space=pltpu.HBM),
            pl.BlockSpec(memory_space=pltpu.HBM),
        ],
        out_specs=(
            pl.BlockSpec(memory_space=pl.ANY),
            pl.BlockSpec(memory_space=pltpu.VMEM),
        ),
        scratch_shapes=[
            [pltpu.VMEM((depth, azimuth + PAD, vertical), jnp.float32)] * chunks,
            pltpu.VMEM((chunks, depth, azimuth, vertical), jnp.float32),
            pltpu.VMEM((2, vertical), jnp.float32),
            pltpu.VMEM((n, 2, vertical), jnp.float32),
            pltpu.VMEM((2, vertical), jnp.float32),
            pltpu.VMEM((m, 2, vertical), jnp.float32),
            DMA((chunks,)),
            DMA((chunks,)),
            DMA((chunks,)),
            DMA((chunks,)),
            DMA,
            DMA,
            DMA,
            DMA,
            pltpu.SMEM((columns,), jnp.int32),
            pltpu.SMEM((columns,), jnp.float32),
            DMA((2,)),
        ],
        compiler_params=pltpu.CompilerParams(
            collective_id=0, has_side_effects=True, vmem_limit_bytes=16 * 2**20
        ),
        cost_estimate=pl.CostEstimate(
            flops=12 * fields.size, bytes_accessed=8 * fields.size, transcendentals=0
        ),
    )(*(pltpu.with_memory_space_constraint(a, pltpu.HBM) for a in (shifts, fraction, fields)))


def solution(mesh):
    in_specs = (P(None, "gx", "gy", None), P("gx"), P("gx"))
    out_specs = (P(None, "gx", "gy", None), P())
    return jax.shard_map(
        on_device, mesh=mesh, in_specs=in_specs, out_specs=out_specs, check_vma=False
    )
```

```python
from functools import partial
import math

import jax
import jax.numpy as jnp
from jax import lax
from jax.experimental import pallas as pl
from jax.experimental.pallas import tpu as pltpu
from jax.sharding import PartitionSpec as P

MESH = pl.DeviceIdType.MESH
FIRST_FIELDS = (1, 2, 5, 6)
TILE = 32
PAD = TILE + 8


def taps_of(share):
    half = 0.5 * share * share
    bend = half * (1.0 - 2.0 * share / 3.0)
    right = (share - half - 3.0 * bend) * (1.0 / 12.0)
    left = (half - 3.0 * bend) * (1.0 / 12.0)
    return (
        -left,
        8.0 * left - right,
        8.0 * right + 6.0 * bend,
        1.0 - 8.0 * left - 6.0 * bend,
        left - 8.0 * right,
        right,
    )


def kernel(
    plan, shifts_in, fraction_in, fields, remapped, stress, held, moved, part, part_y,
    sums, part_x, send1, recv1, send2, recv2, ysend, yrecv, xsend, xrecv, shifts,
    fraction, small_sem,
):
    n, m, components, chunks, depth, per_device, slab, azimuth, scale = plan
    me = lax.axis_index("gy")
    my_x = lax.axis_index("gx")
    order = FIRST_FIELDS + tuple(
        f for f in range(components) if f not in FIRST_FIELDS
    )

    def column_of(device):
        return device * per_device // components

    def field_of(device, chunk):
        if per_device >= components:
            return order[chunk]
        return lax.rem(lax.rem(device * per_device, components) + chunk + 1, components)

    def peer(step):
        away = lax.div(step, 2) * (1 - 2 * lax.rem(step, 2))
        return lax.rem(me + n // 2 + away, n)

    small = (
        pltpu.make_async_copy(shifts_in, shifts, small_sem.at[0]),
        pltpu.make_async_copy(fraction_in, fraction, small_sem.at[1]),
    )
    barrier = pltpu.get_barrier_semaphore()

    def greet_y(step, carry):
        pl.semaphore_signal(
            barrier, inc=1, device_id={"gy": peer(step)}, device_id_type=MESH
        )
        return carry

    lax.fori_loop(1, n, greet_y, 0)
    for step in range(1, m):
        pl.semaphore_signal(
            barrier,
            inc=1,
            device_id={"gx": lax.rem(my_x + step, m)},
            device_id_type=MESH,
        )

    def own_in(chunk):
        return pltpu.make_async_copy(
            fields.at[field_of(me, chunk), pl.ds(column_of(me), depth)],
            held[chunk].at[:, pl.ds(me * slab, slab)],
            recv1.at[chunk],
        )

    for copy in small:
        copy.start()
    for chunk in range(chunks):
        own_in(chunk).start()
    pl.semaphore_wait(barrier, n - 1 + m - 1)

    for chunk in range(chunks):

        def send_in(step, carry):
            to = peer(step)
            pltpu.make_async_remote_copy(
                src_ref=fields.at[field_of(to, chunk), pl.ds(column_of(to), depth)],
                dst_ref=held[chunk].at[:, pl.ds(me * slab, slab)],
                send_sem=send1.at[chunk],
                recv_sem=recv1.at[chunk],
                device_id={"gy": to},
                device_id_type=MESH,
            ).start()
            return carry

        lax.fori_loop(1, n, send_in, 0)

    def whole(chunk):
        return held[chunk].at[:, pl.ds(0, azimuth)]

    def others(chunk):
        return held[chunk].at[:, pl.ds(0, azimuth - slab)]

    def remap(chunk):
        for c in range(depth):
            column = column_of(me) + c
            shift = shifts[column]
            taps = taps_of(fraction[column])
            held[chunk][c, pl.ds(azimuth, PAD)] = held[chunk][c, pl.ds(0, PAD)]

            def tile(t, carry):
                start = lax.rem(t * TILE - 3 - shift + 2 * azimuth, azimuth)
                total = None
                for k in range(6):
                    term = taps[k] * held[chunk][c, pl.ds(start + k, TILE)]
                    total = term if total is None else total + term
                moved[chunk, c, pl.ds(pl.multiple_of(t * TILE, TILE), TILE)] = total
                return carry

            lax.fori_loop(0, azimuth // TILE, tile, 0)

    def own_out(chunk):
        return pltpu.make_async_copy(
            moved.at[chunk, :, pl.ds(me * slab, slab)],
            remapped.at[field_of(me, chunk), pl.ds(column_of(me), depth)],
            recv2.at[chunk],
        )

    def pair_sum(chunk):
        def add(t, total):
            rows = pl.ds(pl.multiple_of(t * 8, 8), 8)
            for c in range(depth):
                total = total + moved[chunk, c, rows] * moved[chunk + 1, c, rows]
            return total

        total = lax.fori_loop(
            0, azimuth // 8, add, jnp.zeros((8, moved.shape[-1]), jnp.float32)
        )
        return jnp.sum(total, axis=0, keepdims=True)

    def start_sums():
        if per_device >= components:
            part[0:1] = pair_sum(0)
            part[1:2] = -pair_sum(2)
        else:
            first = jnp.zeros((1, moved.shape[-1]), jnp.float32)
            second = first
            for chunk in range(0, chunks, 2):
                total = pair_sum(chunk)
                field = field_of(me, chunk)
                first = first + jnp.where(field == 1, total, 0.0)
                second = second - jnp.where(field == 5, total, 0.0)
            part[0:1] = first
            part[1:2] = second
        part_y[pl.ds(me, 1)] = part[...][None]

        def send_sum(step, carry):
            pltpu.make_async_remote_copy(
                src_ref=part,
                dst_ref=part_y.at[me],
                send_sem=ysend,
                recv_sem=yrecv,
                device_id={"gy": peer(step)},
                device_id_type=MESH,
            ).start()
            return carry

        lax.fori_loop(1, n, send_sum, 0)

    for copy in small:
        copy.wait()
    sums_at = min(3, chunks - 1) if per_device >= components else chunks - 1
    for chunk in range(chunks):
        pltpu.make_async_copy(whole(chunk), whole(chunk), recv1.at[chunk]).wait()
        remap(chunk)

        def send_out(step, carry):
            to = peer(step)
            pltpu.make_async_remote_copy(
                src_ref=moved.at[chunk, :, pl.ds(to * slab, slab)],
                dst_ref=remapped.at[field_of(me, chunk), pl.ds(column_of(me), depth)],
                send_sem=send2.at[chunk],
                recv_sem=recv2.at[chunk],
                device_id={"gy": to},
                device_id_type=MESH,
            ).start()
            return carry

        lax.fori_loop(1, n, send_out, 0)
        own_out(chunk).start()
        if chunk == sums_at:
            start_sums()

    few = part_y.at[pl.ds(0, n - 1)]
    pltpu.make_async_copy(few, few, yrecv).wait()
    pltpu.make_async_copy(few, few, ysend).wait()
    sums[...] = jnp.sum(part_y[...], axis=0)
    part_x[pl.ds(my_x, 1)] = sums[...][None]
    for step in range(1, m):
        pltpu.make_async_remote_copy(
            src_ref=sums,
            dst_ref=part_x.at[my_x],
            send_sem=xsend,
            recv_sem=xrecv,
            device_id={"gx": lax.rem(my_x + step, m)},
            device_id_type=MESH,
        ).start()
    rest = part_x.at[pl.ds(0, m - 1)]
    pltpu.make_async_copy(rest, rest, xrecv).wait()
    pltpu.make_async_copy(rest, rest, xsend).wait()
    stress[...] = jnp.sum(part_x[...], axis=0) * scale

    for chunk in range(chunks):
        pltpu.make_async_copy(others(chunk), others(chunk), send1.at[chunk]).wait()
        pltpu.make_async_copy(others(chunk), others(chunk), send2.at[chunk]).wait()
        pltpu.make_async_copy(whole(chunk), whole(chunk), recv2.at[chunk]).wait()


def write_out(landed, sums, remapped, stress, done):
    copies = [
        pltpu.make_async_copy(landed.at[f], remapped.at[f], done.at[f])
        for f in range(landed.shape[0])
    ]
    copies.append(pltpu.make_async_copy(sums, stress, done.at[landed.shape[0]]))
    for copy in copies:
        copy.start()
    for copy in copies:
        copy.wait()


def on_device(fields, shifts, fraction):
    components, columns, slab, vertical = fields.shape
    n = lax.axis_size("gy")
    m = lax.axis_size("gx")
    azimuth = slab * n
    per_device = components * columns // n
    chunks = min(per_device, components)
    depth = max(1, per_device // components)
    scale = 1.0 / math.sqrt(columns * m * azimuth)
    plan = (n, m, components, chunks, depth, per_device, slab, azimuth, scale)
    DMA = pltpu.SemaphoreType.DMA
    landed, sums = pl.pallas_call(
        partial(kernel, plan),
        out_shape=(
            jax.ShapeDtypeStruct(fields.shape, jnp.float32),
            jax.ShapeDtypeStruct((2, vertical), jnp.float32),
        ),
        in_specs=[
            pl.BlockSpec(memory_space=pltpu.HBM),
            pl.BlockSpec(memory_space=pltpu.HBM),
            pl.BlockSpec(memory_space=pltpu.HBM),
        ],
        out_specs=(
            pl.BlockSpec(memory_space=pl.ANY),
            pl.BlockSpec(memory_space=pltpu.VMEM),
        ),
        scratch_shapes=[
            [pltpu.VMEM((depth, azimuth + PAD, vertical), jnp.float32)] * chunks,
            pltpu.VMEM((chunks, depth, azimuth, vertical), jnp.float32),
            pltpu.VMEM((2, vertical), jnp.float32),
            pltpu.VMEM((n, 2, vertical), jnp.float32),
            pltpu.VMEM((2, vertical), jnp.float32),
            pltpu.VMEM((m, 2, vertical), jnp.float32),
            DMA((chunks,)),
            DMA((chunks,)),
            DMA((chunks,)),
            DMA((chunks,)),
            DMA,
            DMA,
            DMA,
            DMA,
            pltpu.SMEM((columns,), jnp.int32),
            pltpu.SMEM((columns,), jnp.float32),
            DMA((2,)),
        ],
        compiler_params=pltpu.CompilerParams(
            collective_id=0, has_side_effects=True, vmem_limit_bytes=16 * 2**20
        ),
        cost_estimate=pl.CostEstimate(
            flops=12 * fields.size, bytes_accessed=8 * fields.size, transcendentals=0
        ),
    )(*(pltpu.with_memory_space_constraint(a, pltpu.HBM) for a in (shifts, fraction, fields)))
    return pl.pallas_call(
        write_out,
        out_shape=(
            jax.ShapeDtypeStruct(fields.shape, jnp.float32),
            jax.ShapeDtypeStruct((2, vertical), jnp.float32),
        ),
        in_specs=[pl.BlockSpec(memory_space=pl.ANY)] * 2,
        out_specs=(pl.BlockSpec(memory_space=pl.ANY),) * 2,
        scratch_shapes=[DMA((components + 1,))],
        compiler_params=pltpu.CompilerParams(vmem_limit_bytes=16 * 2**20),
        cost_estimate=pl.CostEstimate(
            flops=0, bytes_accessed=8 * fields.size, transcendentals=0
        ),
    )(landed, sums)


def solution(mesh):
    in_specs = (P(None, "gx", "gy", None), P("gx"), P("gx"))
    out_specs = (P(None, "gx", "gy", None), P())
    return jax.shard_map(
        on_device, mesh=mesh, in_specs=in_specs, out_specs=out_specs, check_vma=False
    )
```
